32 devices in a mesh: seq: 8 (over y, x, core), tp: 4 (over z).
Axes of the slice: x: 2, y: 2, z: 4, core: 2. Of those that a mesh axis runs over, the one named last changes fastest.
Arguments:
- states: bfloat16 [8, 128, 2048], P('seq', None, 'tp'), may hold values from -60 to 60, as said below
- cotangent: bfloat16 [8, 128, 2048], P('seq', None, 'tp'), may hold values from -12 to 12, as said below
- wq: bfloat16 [2048, 2048], P(None, 'tp'), may hold values from -0.125 to 0.125
- wk: bfloat16 [2048, 512], P(None, 'tp'), may hold values from -0.125 to 0.125
- wv: bfloat16 [2048, 512], P(None, 'tp'), may hold values from -0.125 to 0.125
- wo: bfloat16 [2048, 2048], P('tp'), may hold values from -0.125 to 0.125
Outputs:
- gram: float32 [8, 8], P('seq')
The draws below stay inside these ranges and needn't reach their ends.
Inputs may be any that keep to these rules, and one draw needn't show every extreme that they name: `states`: finite values. `cotangent`: finite values.
All inputs are finite; a program needn't handle non-finite values.
Results may differ from the reference program's by a relative error of at most 0.0025.
Values may be sent and summed in bfloat16 or wider, within the bound.
A program may use at most 64 MiB of HBM per device.

```python
import jax
import jax.numpy as jnp
from jax import lax

D = 2048
HEADS = 32
KV_HEADS = 8
HEAD_DIM = 64
TOKENS_PER_SEQ = 128
SEQUENCE_COUNT = 8


def candidate_rows(key):
    pick_key = jax.random.fold_in(key, 17)
    picked = jax.random.randint(pick_key, (SEQUENCE_COUNT, TOKENS_PER_SEQ), 0, 2).astype(jnp.int32)
    return picked + 2 * jnp.arange(TOKENS_PER_SEQ, dtype=jnp.int32)[None, :]


def draw_states(key, part):
    row_index = candidate_rows(key)
    table_key = jax.random.fold_in(key, 301)
    noise_key = jax.random.fold_in(key, 302)
    candidates = jax.random.normal(table_key, (2 * TOKENS_PER_SEQ, D), jnp.float32)
    noise = 0.4 * jax.random.normal(noise_key, (SEQUENCE_COUNT, TOKENS_PER_SEQ, D), jnp.float32)
    tokens_base = jnp.take(candidates, row_index, axis=0)
    return jnp.clip(tokens_base + noise, -12.0, 12.0).astype(jnp.bfloat16)


def draw_cotangent(key, part):
    row_index = candidate_rows(key)
    table_key = jax.random.fold_in(key, 401)
    noise_key = jax.random.fold_in(key, 402)
    candidates = jax.random.normal(table_key, (2 * TOKENS_PER_SEQ, D), jnp.float32)
    noise = 0.4 * jax.random.normal(noise_key, (SEQUENCE_COUNT, TOKENS_PER_SEQ, D), jnp.float32)
    tokens_base = jnp.take(candidates, row_index, axis=0)
    return jnp.clip(tokens_base + noise, -12.0, 12.0).astype(jnp.bfloat16)


def shard_levels(own_key, shape, cuts, low, high):
    def one(axis_at, parts):
        draws = jax.random.uniform(jax.random.fold_in(jax.random.fold_in(own_key, 6), axis_at), (parts,), jnp.float32, low / len(cuts), high / len(cuts))
        return jnp.repeat(jnp.exp(draws), shape[axis_at] // parts).reshape((-1,) + (1,) * (len(shape) - axis_at - 1))

    gain = one(*cuts[0])
    for cut in cuts[1:]:
        gain = gain * one(*cut)
    return gain


def centred(rng, extent, deviation, limit, shards=(), kind=jnp.bfloat16):
    drawn = deviation * jax.random.normal(rng, extent, jnp.float32)
    if shards:
        drawn = drawn * shard_levels(rng, extent, shards, -0.22, 0.18)
    return jnp.clip(drawn, -limit, limit).astype(kind)


def setup_inputs(seed: int = 0) -> dict:
    seeds = jax.random.split(jax.random.key(seed), 7)
    return {
        "states": draw_states(jax.random.fold_in(seeds[6], 71), 0),
        "cotangent": draw_cotangent(jax.random.fold_in(seeds[6], 71), 0),
        "wq": centred(seeds[2], (D, D), D ** -0.5, 0.125, ((1, 4),)),
        "wk": centred(seeds[3], (D, KV_HEADS * HEAD_DIM), D ** -0.5, 0.125, ((1, 4),)),
        "wv": centred(seeds[4], (D, KV_HEADS * HEAD_DIM), D ** -0.5, 0.125, ((1, 4),)),
        "wo": centred(seeds[5], (D, D), D ** -0.5, 0.125, ((0, 4),)),
    }


theta_base = 500000.0

def rope_tables(length, head_dim):
    half_dim = head_dim // 2
    freqs_k = theta_base ** (-(jnp.arange(half_dim, dtype=jnp.float32) * 2.0 / head_dim))
    angles = jnp.arange(length, dtype=jnp.float32)[:, None] * freqs_k[None, :]
    angles = jnp.concatenate([angles, angles], axis=1)
    return (jnp.cos(angles)[:, None, :], jnp.sin(angles)[:, None, :])

def rotate(values_in, cos_table, sine_table):
    half_dim = values_in.shape[-1] // 2
    turned = jnp.concatenate([-values_in[..., half_dim:], values_in[..., :half_dim]], axis=-1)
    return values_in * cos_table + turned * sine_table

def reference(states, cotangent, wq, wk, wv, wo):
    seqs, length, model_width = states.shape
    group_size = HEADS // KV_HEADS
    tok_rows = seqs * length
    cos_table, sine_table = rope_tables(length, HEAD_DIM)
    flat_states = states.reshape(tok_rows, model_width)
    query_heads = jnp.dot(flat_states, wq, preferred_element_type=jnp.float32).reshape(seqs, length, HEADS, HEAD_DIM)
    query_heads = rotate(query_heads, cos_table, sine_table).astype(jnp.bfloat16).reshape(seqs, length, KV_HEADS, group_size, HEAD_DIM)
    key_heads = jnp.dot(flat_states, wk, preferred_element_type=jnp.float32).reshape(seqs, length, KV_HEADS, HEAD_DIM)
    key_heads = rotate(key_heads, cos_table, sine_table).astype(jnp.bfloat16)
    value_heads = jnp.dot(flat_states, wv, preferred_element_type=jnp.float32).astype(jnp.bfloat16).reshape(seqs, length, KV_HEADS, HEAD_DIM)
    scores = jnp.einsum('sqkgd,stkd->skgqt', query_heads.astype(jnp.float32), key_heads.astype(jnp.float32)) * HEAD_DIM ** (-0.5)
    causal = jnp.arange(length)[:, None] >= jnp.arange(length)[None, :]
    scores = jnp.where(causal, scores, -jnp.inf)
    weights_bf = jax.nn.softmax(scores, axis=-1).astype(jnp.bfloat16)
    attended = jnp.einsum('skgqt,stkd->sqkgd', weights_bf.astype(jnp.float32), value_heads.astype(jnp.float32)).astype(jnp.bfloat16).reshape(seqs, length, model_width)
    grad_attended = lax.dot_general(cotangent.reshape(tok_rows, model_width), wo, (((1,), (1,)), ((), ())), preferred_element_type=jnp.float32).astype(jnp.bfloat16).reshape(seqs, length, KV_HEADS, group_size, HEAD_DIM)
    value_gradient = jnp.einsum('skgqt,sqkgd->stkd', weights_bf.astype(jnp.float32), grad_attended.astype(jnp.float32)).astype(jnp.bfloat16).reshape(seqs, length, KV_HEADS * HEAD_DIM)
    states_wide = states.astype(jnp.float32)
    grad_wv = jnp.einsum('std,stv->sdv', states_wide, value_gradient.astype(jnp.float32), precision=lax.Precision.HIGHEST)
    kernel = jnp.einsum('sdv,rdv->sr', grad_wv, grad_wv, precision=lax.Precision.HIGHEST)
    attended_wide = attended.astype(jnp.float32)
    cot_wide = cotangent.astype(jnp.float32)
    block_cols = model_width // 8

    def block_term(begin_col):
        cot_block = lax.dynamic_slice_in_dim(cot_wide, begin_col, block_cols, 2)
        grad_wo = jnp.einsum('std,ste->sde', attended_wide, cot_block, precision=lax.Precision.HIGHEST)
        return jnp.einsum('sde,rde->sr', grad_wo, grad_wo, precision=lax.Precision.HIGHEST)
    starts = (jnp.arange(8) * block_cols).astype(jnp.int32)
    kernel = kernel + lax.optimization_barrier(jnp.sum(lax.map(block_term, starts), axis=0))
    kernel_diag = jnp.diagonal(kernel)
    return kernel / jnp.sqrt(kernel_diag[:, None] * kernel_diag[None, :])
```

```python
import functools

import jax
import jax.numpy as jnp
import numpy as np
from jax import lax
from jax.experimental import pallas as pl
from jax.experimental.pallas import tpu as pltpu
from jax.sharding import PartitionSpec as P

HEADS = 32
KV_HEADS = 8
HEAD_DIM = 64
THETA = 500000.0
LANES = 128
GROUP = HEADS // KV_HEADS
F32, BF16 = jnp.float32, jnp.bfloat16

NT = (((1,), (1,)), ((), ()))
TN = (((0,), (0,)), ((), ()))


def rope_tables(length):
    half = HEAD_DIM // 2
    freqs = np.float32(THETA) ** (-(np.arange(half, dtype=np.float32) * np.float32(2.0 / HEAD_DIM)))
    angles = np.arange(length, dtype=np.float32)[:, None] * freqs[None, :].astype(np.float32)
    cos, sin = np.cos(angles), np.sin(angles)
    return (
        np.concatenate([cos, cos] * 2, axis=1).astype(np.float32),
        np.concatenate([-sin, sin] * 2, axis=1).astype(np.float32),
    )


def dot(a, b, dims=None):
    if dims is None:
        return jnp.dot(a, b, preferred_element_type=F32)
    return lax.dot_general(a, b, dims, preferred_element_type=F32)


def place_of(index, n):
    if n % 8:
        return index
    block, rest = index // 8, index % 8
    row, col, core = rest // 4, (rest // 2) % 2, rest % 2
    return block * 8 + 2 * (2 * row + (row + col) % 2) + core


def index_at(place, n):
    if n % 8:
        return place
    block, rest = place // 8, place % 8
    spot, core = rest // 2, rest % 2
    row = spot // 2
    return block * 8 + 2 * (2 * row + (row + spot) % 2) + core


def kernel(
    n, tp,
    states_ref, cot_ref, cos_ref, sin_ref, wq_hbm, wk_hbm, wv_hbm, wo_hbm,
    out_ref,
    xs, cs, wqb, wkb, wvb, wob, q_acc, k_acc, v_acc, g_acc,
    fs, fc, fac, fin, ad, rs, full, t1, t1_in, t2,
    w_sem, x_snd, x_rcv, p_snd, p_rcv, f_snd, f_rcv,
    rs_snd, rs_rcv, ag_snd, ag_rcv, r1_snd, r1_rcv, r2_snd, r2_rcv,
):
    length, width = states_ref.shape
    kv_cols = k_acc.shape[1]
    half = n // 2
    rows = length // tp
    lanes = t1.shape[1]
    me = lax.axis_index("seq")
    col = lax.axis_index("tp")
    place = place_of(me, n)

    def turn(d):
        return d * (1 - 2 * ((d + 1) % 2))

    def source(d):
        return index_at((place + turn(d) + n) % n, n)

    def target(d):
        return index_at((place - turn(d) + n) % n, n)

    def peer(k):
        return (col + k) % tp

    def each(lo, hi, body):
        if hi - lo <= 8:
            for i in range(lo, hi):
                body(i)
        else:
            lax.fori_loop(lo, hi, lambda i, c: (body(i), c)[1], 0)

    weight_copies = []
    for k in range(tp):
        at = pl.ds(pl.multiple_of(((col - k + tp) % tp) * width, width), width)
        copies = [
            pltpu.make_async_copy(wq_hbm.at[at, :], wqb.at[k], w_sem.at[4 * k]),
            pltpu.make_async_copy(wk_hbm.at[at, :], wkb.at[k], w_sem.at[4 * k + 1]),
            pltpu.make_async_copy(wv_hbm.at[at, :], wvb.at[k], w_sem.at[4 * k + 2]),
            pltpu.make_async_copy(wo_hbm.at[:, at], wob.at[k], w_sem.at[4 * k + 3]),
        ]
        weight_copies.append(copies)

    barrier = pltpu.get_barrier_semaphore()
    for k in range(1, tp):
        pl.semaphore_signal(barrier, inc=1, device_id={"tp": peer(k)})
    each(1, n, lambda o: pl.semaphore_signal(barrier, inc=1, device_id={"seq": (me + o) % n}))
    for copies in weight_copies:
        for c in copies:
            c.start()
    pl.semaphore_wait(barrier, tp - 1 + n - 1)

    def remote(src, dst, snd, rcv, device):
        return pltpu.make_async_remote_copy(
            src_ref=src, dst_ref=dst, send_sem=snd, recv_sem=rcv, device_id=device
        )

    order = sorted(range(1, tp), key=lambda k: min(k, tp - k))
    x_copies = {}
    for k in order:
        to = {"tp": peer(k)}
        x_copies[k] = (
            remote(states_ref, xs.at[k - 1], x_snd.at[0, k - 1], x_rcv.at[0, k - 1], to),
            remote(cot_ref, cs.at[k - 1], x_snd.at[1, k - 1], x_rcv.at[1, k - 1], to),
        )
        for c in x_copies[k]:
            c.start()

    def plane_copies(d):
        to = {"seq": target(d)}
        return (
            remote(states_ref, fs.at[d - 1], p_snd.at[0, d - 1], p_rcv.at[0, d - 1], to),
            remote(cot_ref, fc.at[d - 1], p_snd.at[1, d - 1], p_rcv.at[1, d - 1], to),
        )

    def start_plane(d):
        for c in plane_copies(d):
            c.start()

    each(1, half + 1, start_plane)

    for k in [0] + order:
        for c in weight_copies[k]:
            c.wait()
        if k == 0:
            x, y = states_ref[...], cot_ref[...]
        else:
            for c in x_copies[k]:
                c.wait_recv()
            x, y = xs[k - 1], cs[k - 1]
        for acc, piece in (
            (q_acc, dot(x, wqb[k])),
            (k_acc, dot(x, wkb[k])),
            (v_acc, dot(x, wvb[k])),
            (g_acc, dot(y, wob[k], NT)),
        ):
            if k == 0:
                acc[...] = piece
            else:
                acc[...] += piece

    lane = lax.broadcasted_iota(jnp.int32, (length, LANES), 1)
    low = lane < HEAD_DIM
    first = lane % HEAD_DIM < HEAD_DIM // 2
    cos, sin = cos_ref[...], sin_ref[...]
    causal = lax.broadcasted_iota(jnp.int32, (length, length), 0) >= lax.broadcasted_iota(
        jnp.int32, (length, length), 1
    )

    def swap(v):
        return pltpu.roll(v, HEAD_DIM, 1)

    def rope(v):
        turned = jnp.where(
            first, pltpu.roll(v, LANES - HEAD_DIM // 2, 1), pltpu.roll(v, HEAD_DIM // 2, 1)
        )
        return v * cos + turned * sin

    def halves(v):
        other = swap(v)
        zero = jnp.zeros_like(v)
        return (
            (jnp.where(low, v, zero).astype(BF16), jnp.where(low, zero, other).astype(BF16)),
            (jnp.where(low, other, zero).astype(BF16), jnp.where(low, zero, v).astype(BF16)),
        )

    def attention():
        for b in range(kv_cols // LANES):
            kcut = slice(b * LANES, (b + 1) * LANES)
            keys = halves(rope(k_acc[:, kcut]))
            values = halves(v_acc[:, kcut])
            sums = []
            for g in range(2):
                parts = [None, None]
                for pair in range(GROUP // 2):
                    at = ((b * 2 + g) * (GROUP // 2) + pair) * LANES
                    cut = slice(at, at + LANES)
                    q = rope(q_acc[:, cut]).astype(BF16)
                    ga = g_acc[:, cut].astype(BF16)
                    att = None
                    for side in range(2):
                        s = dot(q, keys[g][side], NT) * HEAD_DIM ** (-0.5)
                        s = jnp.where(causal, s, -jnp.inf)
                        e = jnp.exp(s - jnp.max(s, axis=1, keepdims=True))
                        p = (e / jnp.sum(e, axis=1, keepdims=True)).astype(BF16)
                        a = dot(p, values[g][side])
                        att = a if att is None else att + a
                        u = dot(p, ga, TN)
                        parts[side] = u if parts[side] is None else parts[side] + u
                    fac[:, cut] = att.astype(BF16)
                sums.append(parts)
            grad = jnp.where(
                low, sums[0][0] + swap(sums[0][1]), swap(sums[1][0]) + sums[1][1]
            )
            fac[:, width + b * LANES : width + (b + 1) * LANES] = grad.astype(BF16)

    def fac_copy(d):
        return remote(
            fac, fin.at[d - 1], f_snd.at[d - 1], f_rcv.at[d - 1], {"seq": target(d)}
        )

    def band(k):
        return pl.ds(pl.multiple_of(k * rows, rows), rows)

    def own_pairs():
        ad[0] = dot(states_ref[...], states_ref[...], NT).astype(BF16)
        ad[1] = dot(cot_ref[...], cot_ref[...], NT).astype(BF16)

        def pair(d):
            for c in plane_copies(d):
                c.wait_recv()
            ad[2 * d] = dot(states_ref[...], fs[d - 1], NT).astype(BF16)
            ad[2 * d + 1] = dot(cot_ref[...], fc[d - 1], NT).astype(BF16)

        each(1, half + 1, pair)

    rs_copies = [
        remote(
            ad.at[:, band(peer(k)), :], rs.at[k - 1], rs_snd.at[k - 1], rs_rcv.at[k - 1],
            {"tp": peer(k)},
        )
        for k in range(1, tp)
    ]
    ag_copies = [
        remote(
            full.at[:, band(col), :], full.at[:, band(col), :], ag_snd.at[k - 1],
            ag_rcv.at[k - 1], {"tp": peer(k)},
        )
        for k in range(1, tp)
    ]

    own_pairs()
    for c in rs_copies:
        c.start()
    attention()
    each(1, half + 1, lambda d: fac_copy(d).start())
    for c in rs_copies:
        c.wait_recv()
    total = ad[:, band(col), :].astype(F32)
    for k in range(1, tp):
        total = total + rs[k - 1].astype(F32)
    full[:, band(col), :] = total.astype(BF16)
    for c in ag_copies:
        c.start()
    for c in ag_copies:
        c.wait_recv()

    row_at = lax.broadcasted_iota(jnp.int32, (8, lanes), 0)
    lane_at = lax.broadcasted_iota(jnp.int32, (8, lanes), 1)

    def entry(d, other):
        b = dot(fac[:, width:], other[:, width:], NT)
        c = dot(fac[:, :width], other[:, :width], NT)
        product = full[2 * d].astype(F32) * b + full[2 * d + 1].astype(F32) * c
        return jnp.sum(jnp.sum(product, axis=0, keepdims=True), axis=1, keepdims=True)

    t1[...] = jnp.where((row_at == 0) & (lane_at == me), entry(0, fac), 0.0)

    def score(d):
        fac_copy(d).wait_recv()
        here = (lane_at == source(d)) & (row_at <= jnp.where(d < half, 1, 0))
        t1[...] += jnp.where(here, entry(d, fin.at[d - 1]), 0.0)

    each(1, half + 1, score)

    r1_copies = [
        remote(t1, t1_in.at[k - 1], r1_snd.at[k - 1], r1_rcv.at[k - 1], {"tp": peer(k)})
        for k in range(1, tp)
    ]
    for c in r1_copies:
        c.start()
    for c in r1_copies:
        c.wait_recv()
    whole = t1[...]
    for k in range(1, tp):
        whole = whole + t1_in[k - 1]
    t2[me] = whole

    def r2_copy(o):
        return remote(
            t2.at[me], t2.at[me], r2_snd.at[o - 1], r2_rcv.at[o - 1], {"seq": (me + o) % n}
        )

    each(1, n, lambda o: r2_copy(o).start())
    each(1, n, lambda o: r2_copy(o).wait_recv())

    straight, mirror = t2[:, 0, :], t2[:, 1, :]
    rank = lax.broadcasted_iota(jnp.int32, (n, lanes), 0)
    spot = lax.broadcasted_iota(jnp.int32, (n, lanes), 1)
    eye = rank == spot
    mine = jnp.sum(jnp.where(spot == me, mirror, 0.0), axis=1, keepdims=True)
    mirrored = jnp.sum(jnp.where(eye, mine, 0.0), axis=0, keepdims=True)
    own = jnp.sum(jnp.where(rank == me, straight, 0.0), axis=0, keepdims=True)
    diag = jnp.sum(jnp.where(eye, straight, 0.0), axis=0, keepdims=True)
    own_diag = jnp.sum(
        jnp.where(spot[:1] == me, diag, 0.0), axis=1, keepdims=True
    )
    gram = (own + mirrored) / jnp.sqrt(own_diag * diag)
    out_ref[...] = gram[:, :n]

    for k in order:
        for c in x_copies[k]:
            c.wait_send()
    for c in rs_copies + ag_copies + r1_copies:
        c.wait_send()

    def drain(d):
        for c in plane_copies(d):
            c.wait_send()
        fac_copy(d).wait_send()

    each(1, half + 1, drain)
    each(1, n, lambda o: r2_copy(o).wait_send())


def on_device(n, tp, states, cotangent, wq, wk, wv, wo):
    seq_dev, length, width = states.shape
    assert seq_dev == 1 and n % 2 == 0 and length == LANES
    kv = wk.shape[1]
    half = n // 2
    tiles = 2 * (half + 1)
    lanes = -(-n // LANES) * LANES
    cos, sin = rope_tables(length)
    vmem = pl.BlockSpec(memory_space=pltpu.VMEM)
    hbm = pl.BlockSpec(memory_space=pl.ANY)
    sem = pltpu.SemaphoreType.DMA
    return pl.pallas_call(
        functools.partial(kernel, n, tp),
        out_shape=jax.ShapeDtypeStruct((1, n), F32),
        in_specs=[vmem] * 4 + [hbm] * 4,
        out_specs=vmem,
        scratch_shapes=[
            pltpu.VMEM((tp - 1, length, width), BF16),
            pltpu.VMEM((tp - 1, length, width), BF16),
            pltpu.VMEM((tp, width, wq.shape[1]), BF16),
            pltpu.VMEM((tp, width, kv), BF16),
            pltpu.VMEM((tp, width, kv), BF16),
            pltpu.VMEM((tp, wo.shape[0], width), BF16),
            pltpu.VMEM((length, wq.shape[1]), F32),
            pltpu.VMEM((length, kv), F32),
            pltpu.VMEM((length, kv), F32),
            pltpu.VMEM((length, wo.shape[0]), F32),
            pltpu.VMEM((half, length, width), BF16),
            pltpu.VMEM((half, length, width), BF16),
            pltpu.VMEM((length, width + kv), BF16),
            pltpu.VMEM((half, length, width + kv), BF16),
            pltpu.VMEM((tiles, length, length), BF16),
            pltpu.VMEM((tp - 1, tiles, length // tp, length), BF16),
            pltpu.VMEM((tiles, length, length), BF16),
            pltpu.VMEM((8, lanes), F32),
            pltpu.VMEM((tp - 1, 8, lanes), F32),
            pltpu.VMEM((n, 8, lanes), F32),
            sem((4 * tp,)),
            sem((2, tp - 1)),
            sem((2, tp - 1)),
            sem((2, half)),
            sem((2, half)),
            sem((half,)),
            sem((half,)),
            sem((tp - 1,)),
            sem((tp - 1,)),
            sem((tp - 1,)),
            sem((tp - 1,)),
            sem((tp - 1,)),
            sem((tp - 1,)),
            sem((n - 1,)),
            sem((n - 1,)),
        ],
        compiler_params=pltpu.CompilerParams(
            collective_id=0, has_side_effects=True, vmem_limit_bytes=60 * 1024 * 1024
        ),
        name="ntk_gram",
    )(
        states.reshape(length, width), cotangent.reshape(length, width),
        jnp.asarray(cos), jnp.asarray(sin), wq, wk, wv, wo,
    )


def solution(mesh):
    in_specs = (
        P("seq", None, "tp"),
        P("seq", None, "tp"),
        P(None, "tp"),
        P(None, "tp"),
        P(None, "tp"),
        P("tp", None),
    )
    return jax.shard_map(
        functools.partial(on_device, mesh.shape["seq"], mesh.shape["tp"]),
        mesh=mesh, in_specs=in_specs, out_specs=P("seq", None), check_vma=False,
    )
```

```python
import functools

import jax
import jax.numpy as jnp
import numpy as np
from jax import lax
from jax.experimental import pallas as pl
from jax.experimental.pallas import tpu as pltpu
from jax.sharding import PartitionSpec as P

HEADS = 32
KV_HEADS = 8
HEAD_DIM = 64
THETA = 500000.0
LANES = 128
GROUP = HEADS // KV_HEADS
F32, BF16 = jnp.float32, jnp.bfloat16

NT = (((1,), (1,)), ((), ()))
TN = (((0,), (0,)), ((), ()))


def rope_tables(length):
    half = HEAD_DIM // 2
    freqs = np.float32(THETA) ** (-(np.arange(half, dtype=np.float32) * np.float32(2.0 / HEAD_DIM)))
    angles = np.arange(length, dtype=np.float32)[:, None] * freqs[None, :].astype(np.float32)
    cos, sin = np.cos(angles), np.sin(angles)
    return (
        np.concatenate([cos, cos] * 2, axis=1).astype(np.float32),
        np.concatenate([-sin, sin] * 2, axis=1).astype(np.float32),
    )


def dot(a, b, dims=None):
    if dims is None:
        return jnp.dot(a, b, preferred_element_type=F32)
    return lax.dot_general(a, b, dims, preferred_element_type=F32)


def place_of(index, n):
    if n % 8:
        return index
    block, rest = index // 8, index % 8
    row, col, core = rest // 4, (rest // 2) % 2, rest % 2
    return block * 8 + 2 * (2 * row + (row + col) % 2) + core


def index_at(place, n):
    if n % 8:
        return place
    block, rest = place // 8, place % 8
    spot, core = rest // 2, rest % 2
    row = spot // 2
    return block * 8 + 2 * (2 * row + (row + spot) % 2) + core


def kernel(
    n, tp,
    states_ref, cot_ref, cos_ref, sin_ref, wq_hbm, wk_hbm, wv_hbm, wo_hbm,
    out_ref,
    xs, cs, wqb, wkb, wvb, wob, q_acc, k_acc, v_acc, g_acc,
    fs, fc, att_own, att_in, gv_own, gv_in, probs, ad, rs, full, t1, t1_in, t2,
    w_sem, x_snd, x_rcv, p_snd, p_rcv, a_snd, a_rcv, g_snd, g_rcv,
    rs_snd, rs_rcv, ag_snd, ag_rcv, r1_snd, r1_rcv, r2_snd, r2_rcv,
):
    length, width = states_ref.shape
    kv_cols = k_acc.shape[1]
    half = n // 2
    rows = length // tp
    lanes = t1.shape[1]
    me = lax.axis_index("seq")
    col = lax.axis_index("tp")
    place = place_of(me, n)

    def turn(d):
        return d * (1 - 2 * ((d + 1) % 2))

    def source(d):
        return index_at((place + turn(d) + n) % n, n)

    def target(d):
        return index_at((place - turn(d) + n) % n, n)

    def peer(k):
        return (col + k) % tp

    def each(lo, hi, body):
        if hi - lo <= 8:
            for i in range(lo, hi):
                body(i)
        else:
            lax.fori_loop(lo, hi, lambda i, c: (body(i), c)[1], 0)

    weight_copies = []
    for k in range(tp):
        at = pl.ds(pl.multiple_of(((col - k + tp) % tp) * width, width), width)
        copies = [
            pltpu.make_async_copy(wq_hbm.at[at, :], wqb.at[k], w_sem.at[4 * k]),
            pltpu.make_async_copy(wk_hbm.at[at, :], wkb.at[k], w_sem.at[4 * k + 1]),
            pltpu.make_async_copy(wv_hbm.at[at, :], wvb.at[k], w_sem.at[4 * k + 2]),
            pltpu.make_async_copy(wo_hbm.at[:, at], wob.at[k], w_sem.at[4 * k + 3]),
        ]
        weight_copies.append(copies)

    barrier = pltpu.get_barrier_semaphore()
    for k in range(1, tp):
        pl.semaphore_signal(barrier, inc=1, device_id={"tp": peer(k)})
    each(1, n, lambda o: pl.semaphore_signal(barrier, inc=1, device_id={"seq": (me + o) % n}))
    for copies in weight_copies:
        for c in copies:
            c.start()
    pl.semaphore_wait(barrier, tp - 1 + n - 1)

    def remote(src, dst, snd, rcv, device):
        return pltpu.make_async_remote_copy(
            src_ref=src, dst_ref=dst, send_sem=snd, recv_sem=rcv, device_id=device
        )

    inputs = (states_ref, cot_ref)
    held = (xs, cs)

    def up(which, k):
        src = inputs[which] if k == 1 else held[which].at[k - 2]
        return remote(
            src, held[which].at[k - 1], x_snd.at[which, 0, k - 1], x_rcv.at[which, k - 1],
            {"tp": peer(1)},
        )

    def down(which, k):
        src = inputs[which] if k == 1 else held[which].at[tp - k]
        return remote(
            src, held[which].at[tp - k - 1], x_snd.at[which, 1, k - 1],
            x_rcv.at[which, tp - k - 1], {"tp": peer(tp - 1)},
        )

    def sends_up(k):
        return (col >= k - 1) & (col < tp - 1)

    def sends_down(k):
        return (col + k - 1 < tp) & (col > 0)

    def pass_on(which, k, act):
        @pl.when(sends_up(k))
        def _():
            act(up(which, k))

        @pl.when(sends_down(k))
        def _():
            act(down(which, k))

    def arrivals(k, body):
        pl.when(col >= k)(lambda: body(k))
        pl.when(col + k < tp)(lambda: body(tp - k))

    def await_block(which, k):
        arrivals(
            k,
            lambda slot: remote(
                inputs[which], held[which].at[slot - 1], x_snd.at[which, 0, 0],
                x_rcv.at[which, slot - 1], {"tp": peer(1)},
            ).wait_recv(),
        )

    for which in range(2):
        pass_on(which, 1, lambda c: c.start())

    def plane_copies(d):
        to = {"seq": target(d)}
        return (
            remote(states_ref, fs.at[d - 1], p_snd.at[0, d - 1], p_rcv.at[0, d - 1], to),
            remote(cot_ref, fc.at[d - 1], p_snd.at[1, d - 1], p_rcv.at[1, d - 1], to),
        )

    def start_plane(d):
        for c in plane_copies(d):
            c.start()

    each(1, half + 1, start_plane)

    def project_states(slot):
        for c in weight_copies[slot][:3]:
            c.wait()
        x = states_ref[...] if slot == 0 else xs[slot - 1]
        for acc, w in ((q_acc, wqb), (k_acc, wkb), (v_acc, wvb)):
            piece = dot(x, w[slot])
            acc[...] = piece if slot == 0 else acc[...] + piece

    def project_cot(slot):
        weight_copies[slot][3].wait()
        y = cot_ref[...] if slot == 0 else cs[slot - 1]
        piece = dot(y, wob[slot], NT)
        g_acc[...] = piece if slot == 0 else g_acc[...] + piece

    lane = lax.broadcasted_iota(jnp.int32, (length, LANES), 1)
    low = lane < HEAD_DIM
    first = lane % HEAD_DIM < HEAD_DIM // 2
    cos, sin = cos_ref[...], sin_ref[...]
    causal = lax.broadcasted_iota(jnp.int32, (length, length), 0) >= lax.broadcasted_iota(
        jnp.int32, (length, length), 1
    )

    def swap(v):
        return pltpu.roll(v, HEAD_DIM, 1)

    def rope(v):
        turned = jnp.where(
            first, pltpu.roll(v, LANES - HEAD_DIM // 2, 1), pltpu.roll(v, HEAD_DIM // 2, 1)
        )
        return v * cos + turned * sin

    def halves(v):
        other = swap(v)
        zero = jnp.zeros_like(v)
        return (
            (jnp.where(low, v, zero).astype(BF16), jnp.where(low, zero, other).astype(BF16)),
            (jnp.where(low, other, zero).astype(BF16), jnp.where(low, zero, v).astype(BF16)),
        )

    blocks = [
        (b, g, (b * 2 + g) * (GROUP // 2) + pair)
        for b in range(kv_cols // LANES)
        for g in range(2)
        for pair in range(GROUP // 2)
    ]

    def attend():
        for b, g, at in blocks:
            kcut, cut = slice(b * LANES, (b + 1) * LANES), slice(at * LANES, (at + 1) * LANES)
            keys = halves(rope(k_acc[:, kcut]))
            values = halves(v_acc[:, kcut])
            q = rope(q_acc[:, cut]).astype(BF16)
            att = None
            for side in range(2):
                s = dot(q, keys[g][side], NT) * HEAD_DIM ** (-0.5)
                s = jnp.where(causal, s, -jnp.inf)
                e = jnp.exp(s - jnp.max(s, axis=1, keepdims=True))
                p = (e / jnp.sum(e, axis=1, keepdims=True)).astype(BF16)
                probs[2 * at + side] = p
                a = dot(p, values[g][side])
                att = a if att is None else att + a
            att_own[:, cut] = att.astype(BF16)

    def grad_values():
        sums = {}
        for b, g, at in blocks:
            ga = g_acc[:, at * LANES : (at + 1) * LANES].astype(BF16)
            for side in range(2):
                u = dot(probs[2 * at + side], ga, TN)
                key = (b, g, side)
                sums[key] = sums[key] + u if key in sums else u
        for b in range(kv_cols // LANES):
            grad = jnp.where(
                low,
                sums[b, 0, 0] + swap(sums[b, 0, 1]),
                swap(sums[b, 1, 0]) + sums[b, 1, 1],
            )
            gv_own[:, b * LANES : (b + 1) * LANES] = grad.astype(BF16)

    def att_copy(d):
        return remote(
            att_own, att_in.at[d - 1], a_snd.at[d - 1], a_rcv.at[d - 1], {"seq": target(d)}
        )

    def gv_copy(d):
        return remote(
            gv_own, gv_in.at[d - 1], g_snd.at[d - 1], g_rcv.at[d - 1], {"seq": target(d)}
        )

    def band(k):
        return pl.ds(pl.multiple_of(k * rows, rows), rows)

    def own_pairs():
        ad[0] = dot(states_ref[...], states_ref[...], NT).astype(BF16)
        ad[1] = dot(cot_ref[...], cot_ref[...], NT).astype(BF16)

        def pair(d):
            for c in plane_copies(d):
                c.wait_recv()
            ad[2 * d] = dot(states_ref[...], fs[d - 1], NT).astype(BF16)
            ad[2 * d + 1] = dot(cot_ref[...], fc[d - 1], NT).astype(BF16)

        each(1, half + 1, pair)

    rs_copies = [
        remote(
            ad.at[:, band(peer(k)), :], rs.at[k - 1], rs_snd.at[k - 1], rs_rcv.at[k - 1],
            {"tp": peer(k)},
        )
        for k in range(1, tp)
    ]
    ag_copies = [
        remote(
            full.at[:, band(col), :], full.at[:, band(col), :], ag_snd.at[k - 1],
            ag_rcv.at[k - 1], {"tp": peer(k)},
        )
        for k in range(1, tp)
    ]

    project_states(0)
    project_cot(0)
    for k in range(1, tp):
        if k == tp - 1:
            own_pairs()
            for c in rs_copies:
                c.start()
        await_block(0, k)
        if k < tp - 1:
            pass_on(0, k + 1, lambda c: c.start())
        arrivals(k, project_states)
        if k == tp - 1:
            attend()
            each(1, half + 1, lambda d: att_copy(d).start())
        await_block(1, k)
        if k < tp - 1:
            pass_on(1, k + 1, lambda c: c.start())
        arrivals(k, project_cot)
    grad_values()
    each(1, half + 1, lambda d: gv_copy(d).start())

    for c in rs_copies:
        c.wait_recv()
    total = ad[:, band(col), :].astype(F32)
    for k in range(1, tp):
        total = total + rs[k - 1].astype(F32)
    full[:, band(col), :] = total.astype(BF16)
    for c in ag_copies:
        c.start()
    for c in ag_copies:
        c.wait_recv()

    row_at = lax.broadcasted_iota(jnp.int32, (8, lanes), 0)
    lane_at = lax.broadcasted_iota(jnp.int32, (8, lanes), 1)

    def entry(d, att_other, gv_other):
        b = dot(gv_own[...], gv_other[...], NT)
        c = dot(att_own[...], att_other[...], NT)
        product = full[2 * d].astype(F32) * b + full[2 * d + 1].astype(F32) * c
        return jnp.sum(jnp.sum(product, axis=0, keepdims=True), axis=1, keepdims=True)

    t1[...] = jnp.where((row_at == 0) & (lane_at == me), entry(0, att_own, gv_own), 0.0)

    def score(d):
        att_copy(d).wait_recv()
        gv_copy(d).wait_recv()
        here = (lane_at == source(d)) & (row_at <= jnp.where(d < half, 1, 0))
        t1[...] += jnp.where(here, entry(d, att_in.at[d - 1], gv_in.at[d - 1]), 0.0)

    each(1, half + 1, score)

    r1_copies = [
        remote(t1, t1_in.at[k - 1], r1_snd.at[k - 1], r1_rcv.at[k - 1], {"tp": peer(k)})
        for k in range(1, tp)
    ]
    for c in r1_copies:
        c.start()
    for c in r1_copies:
        c.wait_recv()
    whole = t1[...]
    for k in range(1, tp):
        whole = whole + t1_in[k - 1]
    t2[me] = whole

    def r2_copy(o):
        return remote(
            t2.at[me], t2.at[me], r2_snd.at[o - 1], r2_rcv.at[o - 1], {"seq": (me + o) % n}
        )

    each(1, n, lambda o: r2_copy(o).start())
    each(1, n, lambda o: r2_copy(o).wait_recv())

    straight, mirror = t2[:, 0, :], t2[:, 1, :]
    rank = lax.broadcasted_iota(jnp.int32, (n, lanes), 0)
    spot = lax.broadcasted_iota(jnp.int32, (n, lanes), 1)
    eye = rank == spot
    mine = jnp.sum(jnp.where(spot == me, mirror, 0.0), axis=1, keepdims=True)
    mirrored = jnp.sum(jnp.where(eye, mine, 0.0), axis=0, keepdims=True)
    own = jnp.sum(jnp.where(rank == me, straight, 0.0), axis=0, keepdims=True)
    diag = jnp.sum(jnp.where(eye, straight, 0.0), axis=0, keepdims=True)
    own_diag = jnp.sum(
        jnp.where(spot[:1] == me, diag, 0.0), axis=1, keepdims=True
    )
    gram = (own + mirrored) / jnp.sqrt(own_diag * diag)
    out_ref[...] = gram[:, :n]

    for k in range(1, tp):
        for which in range(2):
            pass_on(which, k, lambda c: c.wait_send())
    for c in rs_copies + ag_copies + r1_copies:
        c.wait_send()

    def drain(d):
        for c in plane_copies(d):
            c.wait_send()
        att_copy(d).wait_send()
        gv_copy(d).wait_send()

    each(1, half + 1, drain)
    each(1, n, lambda o: r2_copy(o).wait_send())


def on_device(n, tp, states, cotangent, wq, wk, wv, wo):
    seq_dev, length, width = states.shape
    assert seq_dev == 1 and n % 2 == 0 and length == LANES
    kv = wk.shape[1]
    half = n // 2
    tiles = 2 * (half + 1)
    lanes = -(-n // LANES) * LANES
    cos, sin = rope_tables(length)
    vmem = pl.BlockSpec(memory_space=pltpu.VMEM)
    hbm = pl.BlockSpec(memory_space=pl.ANY)
    sem = pltpu.SemaphoreType.DMA
    return pl.pallas_call(
        functools.partial(kernel, n, tp),
        out_shape=jax.ShapeDtypeStruct((1, n), F32),
        in_specs=[vmem] * 4 + [hbm] * 4,
        out_specs=vmem,
        scratch_shapes=[
            pltpu.VMEM((tp - 1, length, width), BF16),
            pltpu.VMEM((tp - 1, length, width), BF16),
            pltpu.VMEM((tp, width, wq.shape[1]), BF16),
            pltpu.VMEM((tp, width, kv), BF16),
            pltpu.VMEM((tp, width, kv), BF16),
            pltpu.VMEM((tp, wo.shape[0], width), BF16),
            pltpu.VMEM((length, wq.shape[1]), F32),
            pltpu.VMEM((length, kv), F32),
            pltpu.VMEM((length, kv), F32),
            pltpu.VMEM((length, wo.shape[0]), F32),
            pltpu.VMEM((half, length, width), BF16),
            pltpu.VMEM((half, length, width), BF16),
            pltpu.VMEM((length, width), BF16),
            pltpu.VMEM((half, length, width), BF16),
            pltpu.VMEM((length, kv), BF16),
            pltpu.VMEM((half, length, kv), BF16),
            pltpu.VMEM((width // HEAD_DIM, length, length), BF16),
            pltpu.VMEM((tiles, length, length), BF16),
            pltpu.VMEM((tp - 1, tiles, length // tp, length), BF16),
            pltpu.VMEM((tiles, length, length), BF16),
            pltpu.VMEM((8, lanes), F32),
            pltpu.VMEM((tp - 1, 8, lanes), F32),
            pltpu.VMEM((n, 8, lanes), F32),
            sem((4 * tp,)),
            sem((2, 2, tp - 1)),
            sem((2, tp - 1)),
            sem((2, half)),
            sem((2, half)),
            sem((half,)),
            sem((half,)),
            sem((half,)),
            sem((half,)),
            sem((tp - 1,)),
            sem((tp - 1,)),
            sem((tp - 1,)),
            sem((tp - 1,)),
            sem((tp - 1,)),
            sem((tp - 1,)),
            sem((n - 1,)),
            sem((n - 1,)),
        ],
        compiler_params=pltpu.CompilerParams(
            collective_id=0, has_side_effects=True, vmem_limit_bytes=60 * 1024 * 1024
        ),
        name="ntk_gram",
    )(
        states.reshape(length, width), cotangent.reshape(length, width),
        jnp.asarray(cos), jnp.asarray(sin), wq, wk, wv, wo,
    )


def solution(mesh):
    in_specs = (
        P("seq", None, "tp"),
        P("seq", None, "tp"),
        P(None, "tp"),
        P(None, "tp"),
        P(None, "tp"),
        P("tp", None),
    )
    return jax.shard_map(
        functools.partial(on_device, mesh.shape["seq"], mesh.shape["tp"]),
        mesh=mesh, in_specs=in_specs, out_specs=P("seq", None), check_vma=False,
    )
```

```python
import functools

import jax
import jax.numpy as jnp
import numpy as np
from jax import lax
from jax.experimental import pallas as pl
from jax.experimental.pallas import tpu as pltpu
from jax.sharding import PartitionSpec as P

HEADS = 32
KV_HEADS = 8
HEAD_DIM = 64
THETA = 500000.0
LANES = 128
GROUP = HEADS // KV_HEADS
F32, BF16 = jnp.float32, jnp.bfloat16

NT = (((1,), (1,)), ((), ()))
TN = (((0,), (0,)), ((), ()))


def rope_tables(length):
    half = HEAD_DIM // 2
    freqs = np.float32(THETA) ** (-(np.arange(half, dtype=np.float32) * np.float32(2.0 / HEAD_DIM)))
    angles = np.arange(length, dtype=np.float32)[:, None] * freqs[None, :].astype(np.float32)
    cos, sin = np.cos(angles), np.sin(angles)
    return (
        np.concatenate([cos, cos] * 2, axis=1).astype(np.float32),
        np.concatenate([-sin, sin] * 2, axis=1).astype(np.float32),
    )


def dot(a, b, dims=None):
    if dims is None:
        return jnp.dot(a, b, preferred_element_type=F32)
    return lax.dot_general(a, b, dims, preferred_element_type=F32)


def place_of(index, n):
    if n % 8:
        return index
    block, rest = index // 8, index % 8
    row, col, core = rest // 4, (rest // 2) % 2, rest % 2
    return block * 8 + 2 * (2 * row + (row + col) % 2) + core


def index_at(place, n):
    if n % 8:
        return place
    block, rest = place // 8, place % 8
    spot, core = rest // 2, rest % 2
    row = spot // 2
    return block * 8 + 2 * (2 * row + (row + spot) % 2) + core


def kernel(
    n, tp,
    states_ref, cot_ref, cos_ref, sin_ref, wq_hbm, wk_hbm, wv_hbm, wo_hbm,
    out_ref,
    xs, cs, wqb, wkb, wvb, wob, q_acc, k_acc, v_acc, g_acc,
    fs, fc, att_own, att_in, gv_own, gv_in, probs, ad, rs, full, t2,
    w_sem, x_snd, x_rcv, p_snd, p_rcv, a_snd, a_rcv, g_snd, g_rcv,
    rs_snd, rs_rcv, ag_snd, ag_rcv, r2_snd, r2_rcv,
):
    length, width = states_ref.shape
    kv_cols = k_acc.shape[1]
    half = n // 2
    rows = length // tp
    lanes = t2.shape[3]
    me = lax.axis_index("seq")
    col = lax.axis_index("tp")
    place = place_of(me, n)

    def turn(d):
        return d * (1 - 2 * ((d + 1) % 2))

    def source(d):
        return index_at((place + turn(d) + n) % n, n)

    def target(d):
        return index_at((place - turn(d) + n) % n, n)

    def peer(k):
        return (col + k) % tp

    def each(lo, hi, body):
        if hi - lo <= 8:
            for i in range(lo, hi):
                body(i)
        else:
            lax.fori_loop(lo, hi, lambda i, c: (body(i), c)[1], 0)

    weight_copies = []
    for k in range(tp):
        at = pl.ds(pl.multiple_of(((col - k + tp) % tp) * width, width), width)
        copies = [
            pltpu.make_async_copy(wq_hbm.at[at, :], wqb.at[k], w_sem.at[4 * k]),
            pltpu.make_async_copy(wk_hbm.at[at, :], wkb.at[k], w_sem.at[4 * k + 1]),
            pltpu.make_async_copy(wv_hbm.at[at, :], wvb.at[k], w_sem.at[4 * k + 2]),
            pltpu.make_async_copy(wo_hbm.at[:, at], wob.at[k], w_sem.at[4 * k + 3]),
        ]
        weight_copies.append(copies)

    barrier = pltpu.get_barrier_semaphore()
    for k in range(1, tp):
        pl.semaphore_signal(barrier, inc=1, device_id={"tp": peer(k)})
    each(1, n, lambda o: pl.semaphore_signal(barrier, inc=1, device_id={"seq": (me + o) % n}))
    for copies in weight_copies:
        for c in copies:
            c.start()
    pl.semaphore_wait(barrier, tp - 1 + n - 1)

    def remote(src, dst, snd, rcv, device):
        return pltpu.make_async_remote_copy(
            src_ref=src, dst_ref=dst, send_sem=snd, recv_sem=rcv, device_id=device
        )

    inputs = (states_ref, cot_ref)
    held = (xs, cs)

    def up(which, k):
        src = inputs[which] if k == 1 else held[which].at[k - 2]
        return remote(
            src, held[which].at[k - 1], x_snd.at[which, 0, k - 1], x_rcv.at[which, k - 1],
            {"tp": peer(1)},
        )

    def down(which, k):
        src = inputs[which] if k == 1 else held[which].at[tp - k]
        return remote(
            src, held[which].at[tp - k - 1], x_snd.at[which, 1, k - 1],
            x_rcv.at[which, tp - k - 1], {"tp": peer(tp - 1)},
        )

    def sends_up(k):
        return (col >= k - 1) & (col < tp - 1)

    def sends_down(k):
        return (col + k - 1 < tp) & (col > 0)

    def pass_on(which, k, act):
        @pl.when(sends_up(k))
        def _():
            act(up(which, k))

        @pl.when(sends_down(k))
        def _():
            act(down(which, k))

    def arrivals(k, body):
        pl.when(col >= k)(lambda: body(k))
        pl.when(col + k < tp)(lambda: body(tp - k))

    def await_block(which, k):
        arrivals(
            k,
            lambda slot: remote(
                inputs[which], held[which].at[slot - 1], x_snd.at[which, 0, 0],
                x_rcv.at[which, slot - 1], {"tp": peer(1)},
            ).wait_recv(),
        )

    for which in range(2):
        pass_on(which, 1, lambda c: c.start())

    def plane_copies(d):
        to = {"seq": target(d)}
        return (
            remote(states_ref, fs.at[d - 1], p_snd.at[0, d - 1], p_rcv.at[0, d - 1], to),
            remote(cot_ref, fc.at[d - 1], p_snd.at[1, d - 1], p_rcv.at[1, d - 1], to),
        )

    def start_plane(d):
        for c in plane_copies(d):
            c.start()

    each(1, half + 1, start_plane)

    def project_states(slot):
        for c in weight_copies[slot][:3]:
            c.wait()
        x = states_ref[...] if slot == 0 else xs[slot - 1]
        for acc, w in ((q_acc, wqb), (k_acc, wkb), (v_acc, wvb)):
            piece = dot(x, w[slot])
            acc[...] = piece if slot == 0 else acc[...] + piece

    def project_cot(slot):
        weight_copies[slot][3].wait()
        y = cot_ref[...] if slot == 0 else cs[slot - 1]
        piece = dot(y, wob[slot], NT)
        g_acc[...] = piece if slot == 0 else g_acc[...] + piece

    lane = lax.broadcasted_iota(jnp.int32, (length, LANES), 1)
    low = lane < HEAD_DIM
    first = lane % HEAD_DIM < HEAD_DIM // 2
    cos, sin = cos_ref[...], sin_ref[...]
    causal = lax.broadcasted_iota(jnp.int32, (length, length), 0) >= lax.broadcasted_iota(
        jnp.int32, (length, length), 1
    )

    def swap(v):
        return pltpu.roll(v, HEAD_DIM, 1)

    def rope(v):
        turned = jnp.where(
            first, pltpu.roll(v, LANES - HEAD_DIM // 2, 1), pltpu.roll(v, HEAD_DIM // 2, 1)
        )
        return v * cos + turned * sin

    def halves(v):
        other = swap(v)
        zero = jnp.zeros_like(v)
        return (
            (jnp.where(low, v, zero).astype(BF16), jnp.where(low, zero, other).astype(BF16)),
            (jnp.where(low, other, zero).astype(BF16), jnp.where(low, zero, v).astype(BF16)),
        )

    blocks = [
        (b, g, (b * 2 + g) * (GROUP // 2) + pair)
        for b in range(kv_cols // LANES)
        for g in range(2)
        for pair in range(GROUP // 2)
    ]

    def attend():
        for b, g, at in blocks:
            kcut, cut = slice(b * LANES, (b + 1) * LANES), slice(at * LANES, (at + 1) * LANES)
            keys = halves(rope(k_acc[:, kcut]))
            values = halves(v_acc[:, kcut])
            q = rope(q_acc[:, cut]).astype(BF16)
            att = None
            for side in range(2):
                s = dot(q, keys[g][side], NT) * HEAD_DIM ** (-0.5)
                s = jnp.where(causal, s, -jnp.inf)
                e = jnp.exp(s - jnp.max(s, axis=1, keepdims=True))
                p = (e / jnp.sum(e, axis=1, keepdims=True)).astype(BF16)
                probs[2 * at + side] = p
                a = dot(p, values[g][side])
                att = a if att is None else att + a
            att_own[:, cut] = att.astype(BF16)

    def grad_values():
        sums = {}
        for b, g, at in blocks:
            ga = g_acc[:, at * LANES : (at + 1) * LANES].astype(BF16)
            for side in range(2):
                u = dot(probs[2 * at + side], ga, TN)
                key = (b, g, side)
                sums[key] = sums[key] + u if key in sums else u
        for b in range(kv_cols // LANES):
            grad = jnp.where(
                low,
                sums[b, 0, 0] + swap(sums[b, 0, 1]),
                swap(sums[b, 1, 0]) + sums[b, 1, 1],
            )
            gv_own[:, b * LANES : (b + 1) * LANES] = grad.astype(BF16)

    def att_copy(d):
        return remote(
            att_own, att_in.at[d - 1], a_snd.at[d - 1], a_rcv.at[d - 1], {"seq": target(d)}
        )

    def gv_copy(d):
        return remote(
            gv_own, gv_in.at[d - 1], g_snd.at[d - 1], g_rcv.at[d - 1], {"seq": target(d)}
        )

    def band(k):
        return pl.ds(pl.multiple_of(k * rows, rows), rows)

    def rs_copies(d):
        two = pl.ds(2 * d, 2)
        return [
            remote(
                ad.at[two, band(peer(k)), :], rs.at[k - 1, two], rs_snd.at[k - 1, d],
                rs_rcv.at[k - 1, d], {"tp": peer(k)},
            )
            for k in range(1, tp)
        ]

    def ag_copies(d):
        part = full.at[pl.ds(2 * d, 2), band(col), :]
        return [
            remote(part, part, ag_snd.at[k - 1, d], ag_rcv.at[k - 1, d], {"tp": peer(k)})
            for k in range(1, tp)
        ]

    def multiply(d, states_other, cot_other):
        ad[2 * d] = dot(states_ref[...], states_other[...], NT).astype(BF16)
        ad[2 * d + 1] = dot(cot_ref[...], cot_other[...], NT).astype(BF16)
        for c in rs_copies(d):
            c.start()

    def pair(d):
        for c in plane_copies(d):
            c.wait_recv()
        multiply(d, fs.at[d - 1], fc.at[d - 1])

    def gather_sum(d):
        for c in rs_copies(d):
            c.wait_recv()
        two = pl.ds(2 * d, 2)
        total = ad[two, band(col), :].astype(F32)
        for k in range(1, tp):
            total = total + rs[k - 1, two].astype(F32)
        full[two, band(col), :] = total.astype(BF16)
        for c in ag_copies(d):
            c.start()

    bounds = [1 + (half * k + tp - 2) // (tp - 1) for k in range(tp)]

    project_states(0)
    multiply(0, states_ref, cot_ref)
    project_cot(0)
    for k in range(1, tp):
        last = k == tp - 1
        await_block(0, k)
        if not last:
            pass_on(0, k + 1, lambda c: c.start())
        arrivals(k, project_states)
        if last:
            each(bounds[k - 1], bounds[k], pair)
            attend()
            each(1, half + 1, lambda d: att_copy(d).start())
        await_block(1, k)
        if not last:
            pass_on(1, k + 1, lambda c: c.start())
        arrivals(k, project_cot)
        if not last:
            each(bounds[k - 1], bounds[k], pair)
            each(bounds[k - 2] if k > 1 else 0, bounds[k - 1], gather_sum)
    grad_values()
    each(1, half + 1, lambda d: gv_copy(d).start())
    each(bounds[tp - 3] if tp > 2 else 0, bounds[tp - 1], gather_sum)

    lane_at = lax.broadcasted_iota(jnp.int32, (1, lanes), 1)

    def entry(d, att_other, gv_other):
        b = dot(gv_own[...], gv_other[...], NT)
        c = dot(att_own[...], att_other[...], NT)
        product = full[2 * d].astype(F32) * b + full[2 * d + 1].astype(F32) * c
        return jnp.sum(jnp.sum(product, axis=0, keepdims=True), axis=1, keepdims=True)

    def settle(d):
        for c in ag_copies(d):
            c.wait_recv()

    settle(0)
    t2[col, me] = jnp.where(lane_at == me, entry(0, att_own, gv_own), 0.0)

    def score(d):
        settle(d)
        att_copy(d).wait_recv()
        gv_copy(d).wait_recv()
        value = entry(d, att_in.at[d - 1], gv_in.at[d - 1])
        t2[col, me] += jnp.where(lane_at == source(d), value, 0.0)

    each(1, half + 1, score)

    def r2_copy(o):
        mine = t2.at[col, me]
        to = {"seq": (me + o) % n, "tp": (col + o // n) % tp}
        return remote(mine, mine, r2_snd.at[o - 1], r2_rcv.at[o - 1], to)

    def every(act):
        if n * tp <= 32:
            for o in range(1, n * tp):
                act(r2_copy(o))
        else:
            each(1, n * tp, lambda o: act(r2_copy(o)))

    every(lambda c: c.start())
    every(lambda c: c.wait_recv())

    table = t2[0].reshape(n, lanes)
    for q in range(1, tp):
        table = table + t2[q].reshape(n, lanes)
    rank = lax.broadcasted_iota(jnp.int32, (n, lanes), 0)
    spot = lax.broadcasted_iota(jnp.int32, (n, lanes), 1)
    eye = rank == spot
    column = jnp.sum(jnp.where(spot == me, table, 0.0), axis=1, keepdims=True)
    theirs = eye & (rank != me) & (rank != source(half))
    mirrored = jnp.sum(jnp.where(theirs, column, 0.0), axis=0, keepdims=True)
    own = jnp.sum(jnp.where(rank == me, table, 0.0), axis=0, keepdims=True)
    diag = jnp.sum(jnp.where(eye, table, 0.0), axis=0, keepdims=True)
    own_diag = jnp.sum(jnp.where(lane_at == me, diag, 0.0), axis=1, keepdims=True)
    gram = (own + mirrored) / jnp.sqrt(own_diag * diag)
    out_ref[...] = gram[:, :n]

    for k in range(1, tp):
        for which in range(2):
            pass_on(which, k, lambda c: c.wait_send())

    def drain_sums(d):
        for c in rs_copies(d) + ag_copies(d):
            c.wait_send()

    each(0, half + 1, drain_sums)

    def drain(d):
        for c in plane_copies(d):
            c.wait_send()
        att_copy(d).wait_send()
        gv_copy(d).wait_send()

    each(1, half + 1, drain)
    every(lambda c: c.wait_send())


def on_device(n, tp, states, cotangent, wq, wk, wv, wo):
    seq_dev, length, width = states.shape
    assert seq_dev == 1 and n % 2 == 0 and length == LANES
    kv = wk.shape[1]
    half = n // 2
    tiles = 2 * (half + 1)
    lanes = -(-n // LANES) * LANES
    cos, sin = rope_tables(length)
    vmem = pl.BlockSpec(memory_space=pltpu.VMEM)
    hbm = pl.BlockSpec(memory_space=pl.ANY)
    sem = pltpu.SemaphoreType.DMA
    return pl.pallas_call(
        functools.partial(kernel, n, tp),
        out_shape=jax.ShapeDtypeStruct((1, n), F32),
        in_specs=[vmem] * 4 + [hbm] * 4,
        out_specs=vmem,
        scratch_shapes=[
            pltpu.VMEM((tp - 1, length, width), BF16),
            pltpu.VMEM((tp - 1, length, width), BF16),
            pltpu.VMEM((tp, width, wq.shape[1]), BF16),
            pltpu.VMEM((tp, width, kv), BF16),
            pltpu.VMEM((tp, width, kv), BF16),
            pltpu.VMEM((tp, wo.shape[0], width), BF16),
            pltpu.VMEM((length, wq.shape[1]), F32),
            pltpu.VMEM((length, kv), F32),
            pltpu.VMEM((length, kv), F32),
            pltpu.VMEM((length, wo.shape[0]), F32),
            pltpu.VMEM((half, length, width), BF16),
            pltpu.VMEM((half, length, width), BF16),
            pltpu.VMEM((length, width), BF16),
            pltpu.VMEM((half, length, width), BF16),
            pltpu.VMEM((length, kv), BF16),
            pltpu.VMEM((half, length, kv), BF16),
            pltpu.VMEM((width // HEAD_DIM, length, length), BF16),
            pltpu.VMEM((tiles, length, length), BF16),
            pltpu.VMEM((tp - 1, tiles, length // tp, length), BF16),
            pltpu.VMEM((tiles, length, length), BF16),
            pltpu.VMEM((tp, n, 1, lanes), F32),
            sem((4 * tp,)),
            sem((2, 2, tp - 1)),
            sem((2, tp - 1)),
            sem((2, half)),
            sem((2, half)),
            sem((half,)),
            sem((half,)),
            sem((half,)),
            sem((half,)),
            sem((tp - 1, half + 1)),
            sem((tp - 1, half + 1)),
            sem((tp - 1, half + 1)),
            sem((tp - 1, half + 1)),
            sem((n * tp - 1,)),
            sem((n * tp - 1,)),
        ],
        compiler_params=pltpu.CompilerParams(
            collective_id=0, has_side_effects=True, vmem_limit_bytes=60 * 1024 * 1024
        ),
        name="ntk_gram",
    )(
        states.reshape(length, width), cotangent.reshape(length, width),
        jnp.asarray(cos), jnp.asarray(sin), wq, wk, wv, wo,
    )


def solution(mesh):
    in_specs = (
        P("seq", None, "tp"),
        P("seq", None, "tp"),
        P(None, "tp"),
        P(None, "tp"),
        P(None, "tp"),
        P("tp", None),
    )
    return jax.shard_map(
        functools.partial(on_device, mesh.shape["seq"], mesh.shape["tp"]),
        mesh=mesh, in_specs=in_specs, out_specs=P("seq", None), check_vma=False,
    )
```

```python
import functools

import jax
import jax.numpy as jnp
import numpy as np
from jax import lax
from jax.experimental import pallas as pl
from jax.experimental.pallas import tpu as pltpu
from jax.sharding import PartitionSpec as P

HEADS = 32
KV_HEADS = 8
HEAD_DIM = 64
THETA = 500000.0
LANES = 128
GROUP = HEADS // KV_HEADS
F32, BF16 = jnp.float32, jnp.bfloat16

NT = (((1,), (1,)), ((), ()))
TN = (((0,), (0,)), ((), ()))


def rope_tables(length):
    half = HEAD_DIM // 2
    freqs = np.float32(THETA) ** (-(np.arange(half, dtype=np.float32) * np.float32(2.0 / HEAD_DIM)))
    angles = np.arange(length, dtype=np.float32)[:, None] * freqs[None, :].astype(np.float32)
    cos, sin = np.cos(angles), np.sin(angles)
    return (
        np.concatenate([cos, cos] * 2, axis=1).astype(np.float32),
        np.concatenate([-sin, sin] * 2, axis=1).astype(np.float32),
    )


def dot(a, b, dims=None):
    if dims is None:
        return jnp.dot(a, b, preferred_element_type=F32)
    return lax.dot_general(a, b, dims, preferred_element_type=F32)


def place_of(index, n):
    if n % 8:
        return index
    block, rest = index // 8, index % 8
    row, col, core = rest // 4, (rest // 2) % 2, rest % 2
    return block * 8 + 2 * (2 * row + (row + col) % 2) + core


def index_at(place, n):
    if n % 8:
        return place
    block, rest = place // 8, place % 8
    spot, core = rest // 2, rest % 2
    row = spot // 2
    return block * 8 + 2 * (2 * row + (row + spot) % 2) + core


def kernel(
    n, tp,
    states_ref, cot_ref, cos_ref, sin_ref, wq_hbm, wk_hbm, wv_hbm, wo_hbm,
    out_ref,
    xs, cs, wqb, wkb, wvb, wob, q_acc, k_acc, v_acc, g_acc,
    fs, fc, att_own, att_in, gv_own, gv_in, probs, ad, rs, full, t2,
    w_sem, x_snd, x_rcv, p_snd, p_rcv, a_snd, a_rcv, g_snd, g_rcv,
    rs_snd, rs_rcv, ag_snd, ag_rcv, r2_snd, r2_rcv,
):
    length, width = states_ref.shape
    kv_cols = k_acc.shape[1]
    half = n // 2
    rows = length // tp
    lanes = t2.shape[3]
    me = lax.axis_index("seq")
    col = lax.axis_index("tp")
    place = place_of(me, n)

    def turn(d):
        return d * (1 - 2 * ((d + 1) % 2))

    def source(d):
        return index_at((place + turn(d) + n) % n, n)

    def target(d):
        return index_at((place - turn(d) + n) % n, n)

    def peer(k):
        return (col + k) % tp

    def each(lo, hi, body):
        if hi - lo <= 8:
            for i in range(lo, hi):
                body(i)
        else:
            lax.fori_loop(lo, hi, lambda i, c: (body(i), c)[1], 0)

    weight_copies = []
    for k in range(tp):
        at = pl.ds(pl.multiple_of(((col - k + tp) % tp) * width, width), width)
        copies = [
            pltpu.make_async_copy(wq_hbm.at[at, :], wqb.at[k], w_sem.at[4 * k]),
            pltpu.make_async_copy(wk_hbm.at[at, :], wkb.at[k], w_sem.at[4 * k + 1]),
            pltpu.make_async_copy(wv_hbm.at[at, :], wvb.at[k], w_sem.at[4 * k + 2]),
            pltpu.make_async_copy(wo_hbm.at[:, at], wob.at[k], w_sem.at[4 * k + 3]),
        ]
        weight_copies.append(copies)

    barrier = pltpu.get_barrier_semaphore()
    for k in range(1, tp):
        pl.semaphore_signal(barrier, inc=1, device_id={"tp": peer(k)})
    each(1, n, lambda o: pl.semaphore_signal(barrier, inc=1, device_id={"seq": (me + o) % n}))
    for copies in weight_copies:
        for c in copies:
            c.start()
    pl.semaphore_wait(barrier, tp - 1 + n - 1)

    def remote(src, dst, snd, rcv, device):
        return pltpu.make_async_remote_copy(
            src_ref=src, dst_ref=dst, send_sem=snd, recv_sem=rcv, device_id=device
        )

    inputs = (states_ref, cot_ref)
    held = (xs, cs)

    def up(which, k):
        src = inputs[which] if k == 1 else held[which].at[k - 2]
        return remote(
            src, held[which].at[k - 1], x_snd.at[which, 0, k - 1], x_rcv.at[which, k - 1],
            {"tp": peer(1)},
        )

    def down(which, k):
        src = inputs[which] if k == 1 else held[which].at[tp - k]
        return remote(
            src, held[which].at[tp - k - 1], x_snd.at[which, 1, k - 1],
            x_rcv.at[which, tp - k - 1], {"tp": peer(tp - 1)},
        )

    def sends_up(k):
        return (col >= k - 1) & (col < tp - 1)

    def sends_down(k):
        return (col + k - 1 < tp) & (col > 0)

    def pass_on(which, k, act):
        @pl.when(sends_up(k))
        def _():
            act(up(which, k))

        @pl.when(sends_down(k))
        def _():
            act(down(which, k))

    def arrivals(k, body):
        pl.when(col >= k)(lambda: body(k))
        pl.when(col + k < tp)(lambda: body(tp - k))

    def await_block(which, k):
        arrivals(
            k,
            lambda slot: remote(
                inputs[which], held[which].at[slot - 1], x_snd.at[which, 0, 0],
                x_rcv.at[which, slot - 1], {"tp": peer(1)},
            ).wait_recv(),
        )

    for which in range(2):
        pass_on(which, 1, lambda c: c.start())

    def plane_copies(d):
        to = {"seq": target(d)}
        return (
            remote(states_ref, fs.at[d - 1], p_snd.at[0, d - 1], p_rcv.at[0, d - 1], to),
            remote(cot_ref, fc.at[d - 1], p_snd.at[1, d - 1], p_rcv.at[1, d - 1], to),
        )

    def start_plane(d):
        for c in plane_copies(d):
            c.start()

    each(1, half + 1, start_plane)

    def project_states(slot):
        for c in weight_copies[slot][:3]:
            c.wait()
        x = states_ref[...] if slot == 0 else xs[slot - 1]
        for acc, w in ((q_acc, wqb), (k_acc, wkb), (v_acc, wvb)):
            piece = dot(x, w[slot])
            acc[...] = piece if slot == 0 else acc[...] + piece

    def project_cot(slot):
        weight_copies[slot][3].wait()
        y = cot_ref[...] if slot == 0 else cs[slot - 1]
        piece = dot(y, wob[slot], NT)
        g_acc[...] = piece if slot == 0 else g_acc[...] + piece

    lane = lax.broadcasted_iota(jnp.int32, (length, LANES), 1)
    low = lane < HEAD_DIM
    first = lane % HEAD_DIM < HEAD_DIM // 2
    cos, sin = cos_ref[...], sin_ref[...]
    causal = lax.broadcasted_iota(jnp.int32, (length, length), 0) >= lax.broadcasted_iota(
        jnp.int32, (length, length), 1
    )

    def swap(v):
        return pltpu.roll(v, HEAD_DIM, 1)

    def rope(v):
        turned = jnp.where(
            first, pltpu.roll(v, LANES - HEAD_DIM // 2, 1), pltpu.roll(v, HEAD_DIM // 2, 1)
        )
        return v * cos + turned * sin

    def halves(v):
        other = swap(v)
        zero = jnp.zeros_like(v)
        return (
            (jnp.where(low, v, zero).astype(BF16), jnp.where(low, zero, other).astype(BF16)),
            (jnp.where(low, other, zero).astype(BF16), jnp.where(low, zero, v).astype(BF16)),
        )

    blocks = [
        (b, g, (b * 2 + g) * (GROUP // 2) + pair)
        for b in range(kv_cols // LANES)
        for g in range(2)
        for pair in range(GROUP // 2)
    ]

    part_cols = width // 2

    def attend(part):
        share = len(blocks) // 2
        for b, g, at in blocks[part * share : (part + 1) * share]:
            kcut, cut = slice(b * LANES, (b + 1) * LANES), slice(at * LANES, (at + 1) * LANES)
            keys = halves(rope(k_acc[:, kcut]))
            values = halves(v_acc[:, kcut])
            q = rope(q_acc[:, cut]).astype(BF16)
            att = None
            for side in range(2):
                s = dot(q, keys[g][side], NT) * HEAD_DIM ** (-0.5)
                s = jnp.where(causal, s, -jnp.inf)
                e = jnp.exp(s - jnp.max(s, axis=1, keepdims=True))
                p = (e / jnp.sum(e, axis=1, keepdims=True)).astype(BF16)
                probs[2 * at + side] = p
                a = dot(p, values[g][side])
                att = a if att is None else att + a
            att_own[:, cut] = att.astype(BF16)

    def grad_values():
        sums = {}
        for b, g, at in blocks:
            ga = g_acc[:, at * LANES : (at + 1) * LANES].astype(BF16)
            for side in range(2):
                u = dot(probs[2 * at + side], ga, TN)
                key = (b, g, side)
                sums[key] = sums[key] + u if key in sums else u
        for b in range(kv_cols // LANES):
            grad = jnp.where(
                low,
                sums[b, 0, 0] + swap(sums[b, 0, 1]),
                swap(sums[b, 1, 0]) + sums[b, 1, 1],
            )
            gv_own[:, b * LANES : (b + 1) * LANES] = grad.astype(BF16)

    def att_copy(d, part):
        cut = pl.ds(part * part_cols, part_cols)
        return remote(
            att_own.at[:, cut], att_in.at[d - 1, :, cut], a_snd.at[part, d - 1],
            a_rcv.at[part, d - 1], {"seq": target(d)},
        )

    def gv_copy(d):
        return remote(
            gv_own, gv_in.at[d - 1], g_snd.at[d - 1], g_rcv.at[d - 1], {"seq": target(d)}
        )

    def band(k):
        return pl.ds(pl.multiple_of(k * rows, rows), rows)

    def rs_copies(d):
        two = pl.ds(2 * d, 2)
        return [
            remote(
                ad.at[two, band(peer(k)), :], rs.at[k - 1, two], rs_snd.at[k - 1, d],
                rs_rcv.at[k - 1, d], {"tp": peer(k)},
            )
            for k in range(1, tp)
        ]

    def ag_copies(d):
        part = full.at[pl.ds(2 * d, 2), band(col), :]
        return [
            remote(part, part, ag_snd.at[k - 1, d], ag_rcv.at[k - 1, d], {"tp": peer(k)})
            for k in range(1, tp)
        ]

    def multiply(d, states_other, cot_other):
        ad[2 * d] = dot(states_ref[...], states_other[...], NT).astype(BF16)
        ad[2 * d + 1] = dot(cot_ref[...], cot_other[...], NT).astype(BF16)
        for c in rs_copies(d):
            c.start()

    def pair(d):
        for c in plane_copies(d):
            c.wait_recv()
        multiply(d, fs.at[d - 1], fc.at[d - 1])

    def gather_sum(d):
        for c in rs_copies(d):
            c.wait_recv()
        two = pl.ds(2 * d, 2)
        total = ad[two, band(col), :].astype(F32)
        for k in range(1, tp):
            total = total + rs[k - 1, two].astype(F32)
        full[two, band(col), :] = total.astype(BF16)
        for c in ag_copies(d):
            c.start()

    bounds = [1 + (half * k + tp - 2) // (tp - 1) for k in range(tp)]

    project_states(0)
    multiply(0, states_ref, cot_ref)
    project_cot(0)
    for k in range(1, tp):
        last = k == tp - 1
        await_block(0, k)
        if not last:
            pass_on(0, k + 1, lambda c: c.start())
        arrivals(k, project_states)
        if last:
            each(bounds[k - 1], bounds[k], pair)
            for part in range(2):
                attend(part)
                each(1, half + 1, lambda d: att_copy(d, part).start())
            each(bounds[k - 2] if k > 1 else 0, bounds[k], gather_sum)
        await_block(1, k)
        if not last:
            pass_on(1, k + 1, lambda c: c.start())
        arrivals(k, project_cot)
        if not last:
            each(bounds[k - 1], bounds[k], pair)
            each(bounds[k - 2] if k > 1 else 0, bounds[k - 1], gather_sum)
    grad_values()
    each(1, half + 1, lambda d: gv_copy(d).start())

    lane_at = lax.broadcasted_iota(jnp.int32, (1, lanes), 1)

    def entry(d, att_other, gv_other):
        b = dot(gv_own[...], gv_other[...], NT)
        c = dot(att_own[...], att_other[...], NT)
        product = full[2 * d].astype(F32) * b + full[2 * d + 1].astype(F32) * c
        return jnp.sum(jnp.sum(product, axis=0, keepdims=True), axis=1, keepdims=True)

    def settle(d):
        for c in ag_copies(d):
            c.wait_recv()

    settle(0)
    t2[col, me] = jnp.where(lane_at == me, entry(0, att_own, gv_own), 0.0)

    def score(d):
        settle(d)
        for part in range(2):
            att_copy(d, part).wait_recv()
        gv_copy(d).wait_recv()
        value = entry(d, att_in.at[d - 1], gv_in.at[d - 1])
        t2[col, me] += jnp.where(lane_at == source(d), value, 0.0)

    each(1, half + 1, score)

    def r2_copy(o):
        mine = t2.at[col, me]
        to = {"seq": (me + o) % n, "tp": (col + o // n) % tp}
        return remote(mine, mine, r2_snd.at[o - 1], r2_rcv.at[o - 1], to)

    def every(act):
        if n * tp <= 32:
            for o in range(1, n * tp):
                act(r2_copy(o))
        else:
            each(1, n * tp, lambda o: act(r2_copy(o)))

    every(lambda c: c.start())
    every(lambda c: c.wait_recv())

    table = t2[0].reshape(n, lanes)
    for q in range(1, tp):
        table = table + t2[q].reshape(n, lanes)
    rank = lax.broadcasted_iota(jnp.int32, (n, lanes), 0)
    spot = lax.broadcasted_iota(jnp.int32, (n, lanes), 1)
    eye = rank == spot
    column = jnp.sum(jnp.where(spot == me, table, 0.0), axis=1, keepdims=True)
    theirs = eye & (rank != me) & (rank != source(half))
    mirrored = jnp.sum(jnp.where(theirs, column, 0.0), axis=0, keepdims=True)
    own = jnp.sum(jnp.where(rank == me, table, 0.0), axis=0, keepdims=True)
    diag = jnp.sum(jnp.where(eye, table, 0.0), axis=0, keepdims=True)
    own_diag = jnp.sum(jnp.where(lane_at == me, diag, 0.0), axis=1, keepdims=True)
    gram = (own + mirrored) / jnp.sqrt(own_diag * diag)
    out_ref[...] = gram[:, :n]

    for k in range(1, tp):
        for which in range(2):
            pass_on(which, k, lambda c: c.wait_send())

    def drain_sums(d):
        for c in rs_copies(d) + ag_copies(d):
            c.wait_send()

    each(0, half + 1, drain_sums)

    def drain(d):
        for c in plane_copies(d):
            c.wait_send()
        for part in range(2):
            att_copy(d, part).wait_send()
        gv_copy(d).wait_send()

    each(1, half + 1, drain)
    every(lambda c: c.wait_send())


def on_device(n, tp, states, cotangent, wq, wk, wv, wo):
    seq_dev, length, width = states.shape
    assert seq_dev == 1 and n % 2 == 0 and length == LANES
    kv = wk.shape[1]
    half = n // 2
    tiles = 2 * (half + 1)
    lanes = -(-n // LANES) * LANES
    cos, sin = rope_tables(length)
    vmem = pl.BlockSpec(memory_space=pltpu.VMEM)
    hbm = pl.BlockSpec(memory_space=pl.ANY)
    sem = pltpu.SemaphoreType.DMA
    return pl.pallas_call(
        functools.partial(kernel, n, tp),
        out_shape=jax.ShapeDtypeStruct((1, n), F32),
        in_specs=[vmem] * 4 + [hbm] * 4,
        out_specs=vmem,
        scratch_shapes=[
            pltpu.VMEM((tp - 1, length, width), BF16),
            pltpu.VMEM((tp - 1, length, width), BF16),
            pltpu.VMEM((tp, width, wq.shape[1]), BF16),
            pltpu.VMEM((tp, width, kv), BF16),
            pltpu.VMEM((tp, width, kv), BF16),
            pltpu.VMEM((tp, wo.shape[0], width), BF16),
            pltpu.VMEM((length, wq.shape[1]), F32),
            pltpu.VMEM((length, kv), F32),
            pltpu.VMEM((length, kv), F32),
            pltpu.VMEM((length, wo.shape[0]), F32),
            pltpu.VMEM((half, length, width), BF16),
            pltpu.VMEM((half, length, width), BF16),
            pltpu.VMEM((length, width), BF16),
            pltpu.VMEM((half, length, width), BF16),
            pltpu.VMEM((length, kv), BF16),
            pltpu.VMEM((half, length, kv), BF16),
            pltpu.VMEM((width // HEAD_DIM, length, length), BF16),
            pltpu.VMEM((tiles, length, length), BF16),
            pltpu.VMEM((tp - 1, tiles, length // tp, length), BF16),
            pltpu.VMEM((tiles, length, length), BF16),
            pltpu.VMEM((tp, n, 1, lanes), F32),
            sem((4 * tp,)),
            sem((2, 2, tp - 1)),
            sem((2, tp - 1)),
            sem((2, half)),
            sem((2, half)),
            sem((2, half)),
            sem((2, half)),
            sem((half,)),
            sem((half,)),
            sem((tp - 1, half + 1)),
            sem((tp - 1, half + 1)),
            sem((tp - 1, half + 1)),
            sem((tp - 1, half + 1)),
            sem((n * tp - 1,)),
            sem((n * tp - 1,)),
        ],
        compiler_params=pltpu.CompilerParams(
            collective_id=0, has_side_effects=True, vmem_limit_bytes=60 * 1024 * 1024
        ),
        name="ntk_gram",
    )(
        states.reshape(length, width), cotangent.reshape(length, width),
        jnp.asarray(cos), jnp.asarray(sin), wq, wk, wv, wo,
    )


def solution(mesh):
    in_specs = (
        P("seq", None, "tp"),
        P("seq", None, "tp"),
        P(None, "tp"),
        P(None, "tp"),
        P(None, "tp"),
        P("tp", None),
    )
    return jax.shard_map(
        functools.partial(on_device, mesh.shape["seq"], mesh.shape["tp"]),
        mesh=mesh, in_specs=in_specs, out_specs=P("seq", None), check_vma=False,
    )
```
